32 devices in a mesh: rows: 16 (over z, x, core), cols: 2 (over y).
Axes of the slice: x: 2, y: 2, z: 4, core: 2. Of those that a mesh axis runs over, the one named last changes fastest.
Arguments:
- columns: float32 [512, 16384], P('cols', 'rows'), may hold values from -200 to 200
Outputs:
- orthonormal: float32 [256, 16384], P('cols', 'rows')
- triangle: float32 [256, 512], P('cols')
- trailing: float32 [256, 16384], P('cols', 'rows')
The draws below stay inside these ranges and needn't reach their ends.
All inputs are finite; a program needn't handle non-finite values.
Results may differ from the reference program's by a relative error of at most 0.00008.
Values sent between devices are 32-bit elements; how exact they have to be, the bound alone decides.
A program may use at most 64 MiB of HBM per device.

```python
import math
import jax
import jax.numpy as jnp
from jax import lax

PANEL = 128
COLUMNS = 512
M_ROWS = 16384


def draw_columns(key, part):
    key_normal = jax.random.fold_in(key, 0)
    entries = jnp.clip(jax.random.normal(key_normal, (COLUMNS, M_ROWS), jnp.float32), -4.0, 4.0)
    position = jnp.arange(M_ROWS, dtype=jnp.float32) / max(M_ROWS - 1, 1)
    rising = 1.0 + 2.0 * position
    return (entries * rising[None, :]).astype(jnp.float32)


def setup_inputs(seed: int = 0) -> dict:
    streams_of = jax.random.split(jax.random.key(seed), 2)
    return {
        "columns": draw_columns(jax.random.fold_in(streams_of[1], 71), 0),
    }


precise = lax.Precision.HIGHEST

def product(left, right):
    return jnp.dot(left.astype(jnp.float32), right.astype(jnp.float32), precision=precise, preferred_element_type=jnp.float32)

def gram_matrix(col_block):
    return product(col_block, col_block.T)

def inverse_lower(lower):
    identity = jnp.eye(lower.shape[0], dtype=lower.dtype)
    return lax.linalg.triangular_solve(lower, identity, left_side=True, lower=True)

def reference(columns):
    scaling = math.sqrt(columns.shape[1])
    panel_first = columns[:PANEL]
    remainder = columns[PANEL:]
    lower_first = jnp.linalg.cholesky(gram_matrix(panel_first))
    ortho_first = product(inverse_lower(lower_first), panel_first)
    coupling_first = product(ortho_first, remainder.T)
    remainder = remainder - product(coupling_first.T, ortho_first)
    panel_second = remainder[:PANEL]
    trailing = remainder[PANEL:]
    lower_second = jnp.linalg.cholesky(gram_matrix(panel_second))
    ortho_second = product(inverse_lower(lower_second), panel_second)
    coupling_second = product(ortho_second, trailing.T)
    trailing = trailing - product(coupling_second.T, ortho_second)
    orthonormal = jnp.concatenate([ortho_first, ortho_second], axis=0) * scaling
    zero_block = jnp.zeros((PANEL, PANEL), columns.dtype)
    upper_rows = jnp.concatenate([lower_first.T, coupling_first], axis=1)
    lower_rows = jnp.concatenate([zero_block, lower_second.T, coupling_second], axis=1)
    triangle = jnp.concatenate([upper_rows, lower_rows], axis=0) / scaling
    return (orthonormal, triangle, trailing)
```

```python
import functools
import math

import jax
import jax.numpy as jnp
from jax import lax
from jax.experimental import pallas as pl
from jax.experimental.pallas import tpu as pltpu
from jax.sharding import PartitionSpec as P

PANEL = 128
STRIP = 16
MESH = pl.DeviceIdType.MESH

precise = lax.Precision.HIGHEST


def product(left, right):
    return jnp.dot(left, right, precision=precise, preferred_element_type=jnp.float32)


def contract(left, right, dims):
    return lax.dot_general(
        left, right, (dims, ((), ())), precision=precise, preferred_element_type=jnp.float32
    )


def across_rows(left, right):
    return contract(left, right, ((1,), (1,)))


def pieces(value):
    first = value.astype(jnp.bfloat16)
    rest = value - first.astype(jnp.float32)
    second = rest.astype(jnp.bfloat16)
    third = (rest - second.astype(jnp.float32)).astype(jnp.bfloat16)
    return first, second, third


def strip_update(left, right):
    a, b, c = pieces(left)
    d, e, f = pieces(right)
    lhs = jnp.concatenate([a, a, b, a, c, b], axis=0)
    rhs = jnp.concatenate([d, e, d, f, d, e], axis=0)
    return lax.dot_general(
        lhs, rhs, (((0,), (0,)), ((), ())), preferred_element_type=jnp.float32
    )


def eliminate(ref, hooks):
    size = ref.shape[0]
    lanes = size
    parts = ref.shape[1] // lanes
    below = lax.broadcasted_iota(jnp.int32, (STRIP, lanes), 0)
    for s in range(size // STRIP):
        at = s * STRIP
        rows = [ref[at:at + STRIP, q * lanes:(q + 1) * lanes] for q in range(parts)]
        cols = [
            jnp.broadcast_to(rows[0][:, at + j:at + j + 1], (STRIP, lanes))
            for j in range(STRIP)
        ]
        for i in range(STRIP):
            pivot = cols[i][i:i + 1]
            inv = lax.rsqrt(pivot)
            inv = inv * (1.5 - 0.5 * pivot * inv * inv)
            col = cols[i] * inv
            coef = jnp.where(below > i, col, 0.0)
            for j in range(i + 1, STRIP):
                cols[j] = cols[j] - coef * col[j:j + 1]
            for q in range(parts):
                row = rows[q][i:i + 1] * inv
                rows[q] = jnp.where(below == i, row, rows[q] - coef * row)
        for q in range(parts):
            ref[at:at + STRIP, q * lanes:(q + 1) * lanes] = rows[q]
        after = at + STRIP
        if after < size:
            update = strip_update(rows[0], jnp.concatenate(rows, axis=1))
            ref[after:, :] = ref[after:, :] - update[after:, :]
        if s in hooks:
            hooks[s]()


def kernel(row_count, scaling, x_ref, ortho_ref, tri_ref, trail_ref,
           xs, a2, part, gram, pair_in, ring_in, both, first, second,
           xy, xy_pair, xy_ring, send, recv_x, recv_pair, recv_ring, recv_all,
           recv_half, recv_y):
    r = lax.axis_index("rows")
    c = lax.axis_index("cols")
    other = 1 - c
    parity = lax.rem(r, 2)
    h = r // 2
    mates = row_count // 2
    partner = (r + 1 - 2 * parity, c)
    across = (r, other)
    size = PANEL

    def mate(k):
        idx = lax.rem(h + k, mates)
        return idx, (idx * 2 + parity, c)

    barrier = pltpu.get_barrier_semaphore()
    for target in [partner, across] + [mate(k)[1] for k in range(1, mates)]:
        pl.semaphore_signal(barrier, inc=1, device_id=target, device_id_type=MESH)
    pl.semaphore_wait(barrier, mates + 1)

    def push(src, dst, send_sem, recv_sem, target):
        return pltpu.make_async_remote_copy(
            src_ref=src, dst_ref=dst, send_sem=send_sem, recv_sem=recv_sem,
            device_id=target, device_id_type=MESH)

    quarter = size // 2

    def x_copy(q):
        return push(x_ref.at[pl.ds(q * quarter, quarter)],
                    xs.at[pl.ds(q * quarter, quarter)],
                    send.at[q], recv_x.at[q], across)

    def a2_copy(q):
        return push(x_ref.at[pl.ds(q * quarter, quarter)],
                    a2.at[pl.ds(q * quarter, quarter)],
                    send.at[q], recv_x.at[q], across)

    @pl.when(c == 0)
    def _():
        x_copy(0).start()
        x_copy(1).start()

    @pl.when(c == 1)
    def _():
        a2_copy(0).start()
        a2_copy(1).start()
        a2[...] = x_ref[size:, :]

    def spread(base, full, pair_buf, ring_buf, tag):
        half = full.shape[0] // 2
        chunk = half // mates
        mine = pl.ds(parity * half, half)
        his = pl.ds((1 - parity) * half, half)
        own = pl.ds(pl.multiple_of(parity * half + h * chunk, 8), chunk)

        def pair_copy():
            return push(full.at[his], pair_buf, send.at[base],
                        recv_pair.at[tag], partner)

        def ring_copy(k):
            idx, target = mate(k)
            return push(
                full.at[pl.ds(pl.multiple_of(parity * half + idx * chunk, 8), chunk)],
                ring_buf.at[k], send.at[base + k], recv_ring.at[tag * mates + k], target)

        def gather_copy(dst, k):
            return push(dst.at[own], dst.at[own], send.at[base + mates + k],
                        recv_all.at[tag * mates + k], mate(k)[1])

        def gather_wait(dst, k):
            idx = lax.rem(h + mates - k, mates)
            there = pl.ds(pl.multiple_of(parity * half + idx * chunk, 8), chunk)
            push(dst.at[there], dst.at[there], send.at[base + mates + k],
                 recv_all.at[tag * mates + k], mate(k)[1]).wait_recv()

        def half_copy(dst):
            return push(dst.at[mine], dst.at[mine], send.at[base + 2 * mates],
                        recv_half.at[tag], partner)

        def half_wait(dst):
            push(dst.at[his], dst.at[his], send.at[base + 2 * mates],
                 recv_half.at[tag], partner).wait_recv()

        def start_pair():
            pair_copy().start()

        def start_ring():
            pair_copy().wait_recv()
            full[mine] = full[mine] + pair_buf[...]
            for k in range(1, mates):
                ring_copy(k).start()

        def finish_ring(dst):
            for k in range(1, mates):
                ring_copy(k).wait_recv()
            total = full[own]
            for k in range(1, mates):
                total = total + ring_buf[k]
            dst[own] = total

        def drain_scatter():
            pair_copy().wait_send()
            for k in range(1, mates):
                ring_copy(k).wait_send()

        def start_gather(dst):
            for k in range(1, mates):
                gather_copy(dst, k).start()

        def start_half(dst):
            for k in range(1, mates):
                gather_wait(dst, k)
            half_copy(dst).start()

        def finish(dst):
            half_wait(dst)

        def drain_gather(dst):
            for k in range(1, mates):
                gather_copy(dst, k).wait_send()
            half_copy(dst).wait_send()

        return (start_pair, start_ring, finish_ring, drain_scatter, start_gather,
                start_half, finish, drain_gather, own)

    base_g = 4
    (g_pair, g_ring, g_sum, g_drain, g_gather, g_half, g_finish, g_drain_all,
     g_own) = spread(base_g, part, pair_in, ring_in, 0)
    base_y = base_g + 2 * mates + 2
    y_send = send.at[base_g + 2 * mates + 1]

    def chunk_copy():
        return push(gram.at[g_own], gram.at[g_own], y_send, recv_y.at[0], across)

    @pl.when(c == 0)
    def _():
        part[:2 * size] = across_rows(x_ref[...], x_ref[:size])
        part[2 * size:] = across_rows(x_ref[size:, :], x_ref[size:, :])
        low = part[size:2 * size]
        part[size:2 * size] = low.T
        g_pair()
        xs[...] = x_ref[...]
        g_ring()
        g_sum(gram)
        chunk_copy().start()
        x_copy(2).start()
        x_copy(3).start()

    @pl.when(c == 1)
    def _():
        chunk_copy().wait_recv()

    g_gather(gram)
    g_half(gram)
    g_finish(gram)

    eye = (lax.broadcasted_iota(jnp.int32, (size, size), 0)
           == lax.broadcasted_iota(jnp.int32, (size, size), 1)).astype(jnp.float32)
    first[:, :size] = gram[:size]
    first[:, size:2 * size] = gram[size:2 * size]
    first[:, 2 * size:] = eye
    eliminate(first, {})

    @pl.when(c == 0)
    def _():
        a2_copy(0).wait_recv()
        a2_copy(1).wait_recv()

    @pl.when(c == 1)
    def _():
        for q in range(4):
            x_copy(q).wait_recv()

    (y_pair, y_ring, y_sum, y_drain, y_gather, y_half, y_finish, y_drain_all,
     _own) = spread(base_y, xy, xy_pair, xy_ring, 1)
    xy[...] = across_rows(xs[...], a2[...])
    y_pair()

    upper = first[:, size:2 * size]
    cross = contract(upper, first[:, size:], ((0,), (0,)))
    second[:, :size] = gram[2 * size:] - cross[:, :size]
    second[:, size:2 * size] = -cross[:, size:]
    second[:, 2 * size:] = eye

    mine_xy = both.at[c]

    def swap_copy():
        return push(both.at[c], both.at[c], send.at[base_y + 2 * mates + 1],
                    recv_y.at[1], across)

    def swap_wait():
        push(both.at[other], both.at[other], send.at[base_y + 2 * mates + 1],
             recv_y.at[1], across).wait_recv()

    def hook_sum():
        y_sum(mine_xy)
        y_gather(mine_xy)

    def hook_swap():
        y_finish(mine_xy)
        swap_copy().start()

    eliminate(second, {0: y_ring, 3: hook_sum, 6: lambda: y_half(mine_xy), 7: hook_swap})

    inv00 = first[:, 2 * size:]
    inv1 = second[:, size:]
    mine = both[c]
    coup0 = product(inv00, mine[:size])
    coup1 = product(inv1, mine)
    weights = contract(coup1, inv1, ((0,), (0,)))
    weights0 = weights[:, :size] + contract(coup0, inv00, ((0,), (0,)))
    trail_ref[...] = a2[...] - (product(weights0, xs[:size]) + product(weights[:, size:], xs[size:]))

    @pl.when(c == 0)
    def _():
        ortho_ref[...] = product(inv00, xs[:size]) * scaling

    @pl.when(c == 1)
    def _():
        ortho_ref[...] = product(inv1, xs[...]) * scaling

    swap_wait()
    keep = (lax.broadcasted_iota(jnp.int32, (size, size), 0)
            <= lax.broadcasted_iota(jnp.int32, (size, size), 1))

    @pl.when(c == 0)
    def _():
        tri_ref[:, :size] = jnp.where(keep, first[:, :size], 0.0) / scaling
        tri_ref[:, size:2 * size] = first[:, size:2 * size] / scaling
        for k in range(2):
            tri_ref[:, (2 + k) * size:(3 + k) * size] = (
                product(inv00, both[k][:size]) / scaling)
        for q in range(4):
            x_copy(q).wait_send()
        g_drain()
        chunk_copy().wait_send()

    @pl.when(c == 1)
    def _():
        tri_ref[:, :size] = jnp.zeros((size, size), jnp.float32)
        tri_ref[:, size:2 * size] = jnp.where(keep, second[:, :size], 0.0) / scaling
        for k in range(2):
            tri_ref[:, (2 + k) * size:(3 + k) * size] = product(inv1, both[k]) / scaling
        for q in range(2):
            a2_copy(q).wait_send()

    g_drain_all(gram)
    y_drain()
    y_drain_all(mine_xy)
    swap_copy().wait_send()


def fused(columns):
    row_count = lax.axis_size("rows")
    width = columns.shape[1]
    scaling = math.sqrt(width * row_count)
    size = PANEL
    mates = row_count // 2
    f32 = jnp.float32
    vmem = pl.BlockSpec(memory_space=pltpu.VMEM)
    return pl.pallas_call(
        functools.partial(kernel, row_count, scaling),
        out_shape=(
            jax.ShapeDtypeStruct((size, width), f32),
            jax.ShapeDtypeStruct((size, 4 * size), f32),
            jax.ShapeDtypeStruct((size, width), f32),
        ),
        in_specs=[vmem],
        out_specs=(vmem, vmem, vmem),
        scratch_shapes=[
            pltpu.VMEM((2 * size, width), f32),
            pltpu.VMEM((size, width), f32),
            pltpu.VMEM((3 * size, size), f32),
            pltpu.VMEM((3 * size, size), f32),
            pltpu.VMEM((3 * size // 2, size), f32),
            pltpu.VMEM((mates, 3 * size // row_count, size), f32),
            pltpu.VMEM((2, 2 * size, size), f32),
            pltpu.VMEM((size, 3 * size), f32),
            pltpu.VMEM((size, 3 * size), f32),
            pltpu.VMEM((2 * size, size), f32),
            pltpu.VMEM((size, size), f32),
            pltpu.VMEM((mates, 2 * size // row_count, size), f32),
            pltpu.SemaphoreType.DMA((4 + 2 * (2 * mates + 2),)),
            pltpu.SemaphoreType.DMA((4,)),
            pltpu.SemaphoreType.DMA((2,)),
            pltpu.SemaphoreType.DMA((2 * mates,)),
            pltpu.SemaphoreType.DMA((2 * mates,)),
            pltpu.SemaphoreType.DMA((2,)),
            pltpu.SemaphoreType.DMA((2,)),
        ],
        compiler_params=pltpu.CompilerParams(collective_id=0, has_side_effects=True),
    )(columns)


def inverse_lower(lower):
    identity = jnp.eye(lower.shape[0], dtype=lower.dtype)
    return lax.linalg.triangular_solve(lower, identity, left_side=True, lower=True)


def summed(partial_term):
    return lax.psum(partial_term, "rows")


def general(columns):
    col_count = lax.axis_size("cols")
    col_index = lax.axis_index("cols")
    scaling = math.sqrt(columns.shape[1] * lax.axis_size("rows"))
    local_rows = lax.all_gather(columns, "cols", axis=0, tiled=True)
    panel_count = 2 * PANEL
    leading = local_rows[:panel_count]
    gram_strip = summed(product(leading, local_rows.T))
    lower_both = jnp.linalg.cholesky(gram_strip[:, :panel_count])
    inverse_both = inverse_lower(lower_both)
    orthonormal = product(inverse_both, leading)
    coupling = product(inverse_both, gram_strip[:, panel_count:])
    trailing = local_rows[panel_count:] - product(coupling.T, orthonormal)
    triangle = jnp.concatenate([lower_both.T, coupling], axis=1)
    orthonormal = orthonormal * scaling
    triangle = triangle / scaling

    def own(array):
        count = array.shape[0] // col_count
        return lax.dynamic_slice_in_dim(array, col_index * count, count, 0)

    return (own(orthonormal), own(triangle), own(trailing))


def shards(columns):
    rows = lax.axis_size("rows")
    paired = lax.axis_size("cols") == 2 and columns.shape[0] == 2 * PANEL
    if paired and rows % 2 == 0 and (2 * PANEL) % (8 * rows) == 0 and (3 * PANEL) % (8 * rows) == 0:
        return fused(columns)
    return general(columns)


def solution(mesh):
    placed = (P("cols", "rows"),)
    return jax.shard_map(
        shards,
        mesh=mesh,
        in_specs=placed,
        out_specs=(P("cols", "rows"), P("cols", None), P("cols", "rows")),
        check_vma=False,
    )
```

```python
import functools
import math

import jax
import jax.numpy as jnp
from jax import lax
from jax.experimental import pallas as pl
from jax.experimental.pallas import tpu as pltpu
from jax.sharding import PartitionSpec as P

PANEL = 128
STRIP = 16
MESH = pl.DeviceIdType.MESH

precise = lax.Precision.HIGHEST


def product(left, right):
    return jnp.dot(left, right, precision=precise, preferred_element_type=jnp.float32)


def contract(left, right, dims):
    return lax.dot_general(
        left, right, (dims, ((), ())), precision=precise, preferred_element_type=jnp.float32
    )


def across_rows(left, right):
    return contract(left, right, ((1,), (1,)))


def pieces(value):
    first = value.astype(jnp.bfloat16)
    rest = value - first.astype(jnp.float32)
    second = rest.astype(jnp.bfloat16)
    third = (rest - second.astype(jnp.float32)).astype(jnp.bfloat16)
    return first, second, third


def strip_update(left, right):
    a, b, c = pieces(left)
    d, e, f = pieces(right)
    lhs = jnp.concatenate([a, a, b, a, c, b], axis=0)
    rhs = jnp.concatenate([d, e, d, f, d, e], axis=0)
    return lax.dot_general(
        lhs, rhs, (((0,), (0,)), ((), ())), preferred_element_type=jnp.float32
    )


def eliminate(ref, hooks):
    size = ref.shape[0]
    lanes = size
    parts = ref.shape[1] // lanes
    below = lax.broadcasted_iota(jnp.int32, (STRIP, lanes), 0)
    for s in range(size // STRIP):
        at = s * STRIP
        rows = [ref[at:at + STRIP, q * lanes:(q + 1) * lanes] for q in range(parts)]
        cols = [
            jnp.broadcast_to(rows[0][:, at + j:at + j + 1], (STRIP, lanes))
            for j in range(STRIP)
        ]
        for i in range(STRIP):
            pivot = cols[i][i:i + 1]
            inv = lax.rsqrt(pivot)
            inv = inv * (1.5 - 0.5 * pivot * inv * inv)
            col = cols[i] * inv
            coef = jnp.where(below > i, col, 0.0)
            for j in range(i + 1, STRIP):
                cols[j] = cols[j] - coef * col[j:j + 1]
            for q in range(parts):
                row = rows[q][i:i + 1] * inv
                rows[q] = jnp.where(below == i, row, rows[q] - coef * row)
        for q in range(parts):
            ref[at:at + STRIP, q * lanes:(q + 1) * lanes] = rows[q]
        after = at + STRIP
        if after < size:
            update = strip_update(rows[0], jnp.concatenate(rows, axis=1))
            ref[after:, :] = ref[after:, :] - update[after:, :]
        if s in hooks:
            hooks[s]()


def kernel(row_count, scaling, x_ref, ortho_ref, tri_ref, trail_ref,
           xs, ys, qs, part, gram, pair_in, ring_in, first, second,
           xy, xy_pair, xy_ring, xy_own, xy_other, coupled, send, recv_x, recv_pair,
           recv_ring, recv_all, recv_half, recv_y):
    r = lax.axis_index("rows")
    c = lax.axis_index("cols")
    other = 1 - c
    parity = lax.rem(r, 2)
    h = r // 2
    mates = row_count // 2
    partner = (r + 1 - 2 * parity, c)
    across = (r, other)
    size = PANEL

    def mate(k):
        idx = lax.rem(h + k, mates)
        return idx, (idx * 2 + parity, c)

    barrier = pltpu.get_barrier_semaphore()
    for target in [partner, across] + [mate(k)[1] for k in range(1, mates)]:
        pl.semaphore_signal(barrier, inc=1, device_id=target, device_id_type=MESH)
    pl.semaphore_wait(barrier, mates + 1)

    def push(src, dst, send_sem, recv_sem, target):
        return pltpu.make_async_remote_copy(
            src_ref=src, dst_ref=dst, send_sem=send_sem, recv_sem=recv_sem,
            device_id=target, device_id_type=MESH)

    width = x_ref.shape[1]
    eighth = width // 8
    early = pl.ds(0, 4 * eighth)
    late = pl.ds(4 * eighth, 4 * eighth)
    spans = ((4, 3), (7, 1), (0, 3), (3, 1))

    def x_copy(q):
        span = pl.ds(spans[q][0] * eighth, spans[q][1] * eighth)
        return push(x_ref.at[:, span], xs.at[:, span], send.at[q], recv_x.at[q], across)

    def y_copy(q):
        view = (pl.ds(0, 2 * size), early) if q == 0 else (pl.ds(0, size), late)
        return push(x_ref.at[view], ys.at[view], send.at[q], recv_x.at[q], across)

    @pl.when(c == 0)
    def _():
        x_copy(0).start()

    @pl.when(c == 1)
    def _():
        y_copy(0).start()
        y_copy(1).start()
        ys[...] = x_ref[...]

    def spread(base, full, pair_buf, ring_buf, tag):
        half = full.shape[0] // 2
        chunk = half // mates
        mine = pl.ds(parity * half, half)
        his = pl.ds((1 - parity) * half, half)
        own = pl.ds(pl.multiple_of(parity * half + h * chunk, 8), chunk)

        def pair_copy():
            return push(full.at[his], pair_buf, send.at[base],
                        recv_pair.at[tag], partner)

        def ring_copy(k):
            idx, target = mate(k)
            return push(
                full.at[pl.ds(pl.multiple_of(parity * half + idx * chunk, 8), chunk)],
                ring_buf.at[k], send.at[base + k], recv_ring.at[tag * mates + k], target)

        def gather_copy(dst, k):
            return push(dst.at[own], dst.at[own], send.at[base + mates + k],
                        recv_all.at[tag * mates + k], mate(k)[1])

        def gather_wait(dst, k):
            idx = lax.rem(h + mates - k, mates)
            there = pl.ds(pl.multiple_of(parity * half + idx * chunk, 8), chunk)
            push(dst.at[there], dst.at[there], send.at[base + mates + k],
                 recv_all.at[tag * mates + k], mate(k)[1]).wait_recv()

        def half_copy(dst):
            return push(dst.at[mine], dst.at[mine], send.at[base + 2 * mates],
                        recv_half.at[tag], partner)

        def half_wait(dst):
            push(dst.at[his], dst.at[his], send.at[base + 2 * mates],
                 recv_half.at[tag], partner).wait_recv()

        def start_pair():
            pair_copy().start()

        def start_ring():
            pair_copy().wait_recv()
            full[mine] = full[mine] + pair_buf[...]
            for k in range(1, mates):
                ring_copy(k).start()

        def finish_ring():
            for k in range(1, mates):
                ring_copy(k).wait_recv()
            total = full[own]
            for k in range(1, mates):
                total = total + ring_buf[k]
            return total

        def drain_scatter():
            pair_copy().wait_send()
            for k in range(1, mates):
                ring_copy(k).wait_send()

        def start_gather(dst):
            for k in range(1, mates):
                gather_copy(dst, k).start()

        def start_half(dst):
            for k in range(1, mates):
                gather_wait(dst, k)
            half_copy(dst).start()

        def finish(dst):
            half_wait(dst)

        def drain_gather(dst):
            for k in range(1, mates):
                gather_copy(dst, k).wait_send()
            half_copy(dst).wait_send()

        return (start_pair, start_ring, finish_ring, drain_scatter, start_gather,
                start_half, finish, drain_gather, own)

    base_g = 4
    (g_pair, g_ring, g_sum, g_drain, g_gather, g_half, g_finish, g_drain_all,
     g_own) = spread(base_g, part, pair_in, ring_in, 0)
    base_y = base_g + 2 * mates + 2
    y_send = send.at[base_g + 2 * mates + 1]

    def chunk_copy():
        return push(gram.at[g_own], gram.at[g_own], y_send, recv_y.at[0], across)

    (y_pair, y_ring, y_sum, y_drain, y_gather, y_half, y_finish, y_drain_all,
     y_own) = spread(base_y, xy, xy_pair, xy_ring, 1)

    @pl.when(c == 0)
    def _():
        strip = across_rows(x_ref[:size], x_ref[...])
        part[:size] = strip[:, :size]
        part[size:2 * size] = strip[:, size:]
        part[2 * size:] = across_rows(x_ref[size:, :], x_ref[size:, :])
        g_pair()
        xs[...] = x_ref[...]
        g_ring()
        gram[g_own] = g_sum()
        chunk_copy().start()
        x_copy(1).start()
        x_copy(2).start()

    @pl.when(c == 1)
    def _():
        chunk_copy().wait_recv()

    g_gather(gram)
    g_half(gram)

    @pl.when(c == 0)
    def _():
        y_copy(0).wait_recv()
        xy[...] = across_rows(xs[:, early], ys[:, early])

    @pl.when(c == 1)
    def _():
        x_copy(0).wait_recv()
        x_copy(1).wait_recv()
        xy[...] = across_rows(xs[:, late], ys[:, late])

    y_pair()
    g_finish(gram)

    eye = (lax.broadcasted_iota(jnp.int32, (size, size), 0)
           == lax.broadcasted_iota(jnp.int32, (size, size), 1)).astype(jnp.float32)
    first[:, :size] = gram[:size]
    first[:, size:2 * size] = gram[size:2 * size]
    first[:, 2 * size:] = eye

    def swap_copy():
        return push(xy_own, xy_other, send.at[base_y + 2 * mates + 1], recv_y.at[1], across)

    def hook_sum():
        xy_own[...] = y_sum()
        swap_copy().start()

        @pl.when(c == 0)
        def _():
            x_copy(3).start()

    def hook_gather():
        swap_copy().wait_recv()
        coupled[y_own] = xy_own[...] + xy_other[...]
        y_gather(coupled)

    eliminate(first, {0: y_ring, 6: hook_sum})

    upper = first[:, size:2 * size]
    cross = contract(upper, first[:, size:], ((0,), (0,)))
    second[:, :size] = gram[2 * size:] - cross[:, :size]
    second[:, size:2 * size] = -cross[:, size:]
    second[:, 2 * size:] = eye
    eliminate(second, {0: hook_gather, 7: lambda: y_half(coupled)})

    @pl.when(c == 1)
    def _():
        x_copy(2).wait_recv()
        x_copy(3).wait_recv()

    inv00 = first[:, 2 * size:]
    inv1 = second[:, size:]
    qs[:size] = product(inv00, xs[:size])
    qs[size:] = product(inv1, xs[...])
    own_rows = pl.ds(pl.multiple_of(c * size, size), size)
    ortho_ref[...] = qs[own_rows] * scaling

    @pl.when(c == 0)
    def _():
        y_copy(1).wait_recv()

    y_finish(coupled)
    mine = coupled[:, pl.ds(pl.multiple_of(c * size, size), size)]
    coup = jnp.concatenate([product(inv00, mine[:size]), product(inv1, mine)], axis=0)
    trail_ref[...] = ys[own_rows] - contract(coup, qs[...], ((0,), (0,)))

    keep = (lax.broadcasted_iota(jnp.int32, (size, size), 0)
            <= lax.broadcasted_iota(jnp.int32, (size, size), 1))

    @pl.when(c == 0)
    def _():
        tri_ref[:, :size] = jnp.where(keep, first[:, :size], 0.0) / scaling
        tri_ref[:, size:2 * size] = first[:, size:2 * size] / scaling
        tri_ref[:, 2 * size:] = product(inv00, coupled[:size]) / scaling
        for q in range(4):
            x_copy(q).wait_send()
        g_drain()
        chunk_copy().wait_send()

    @pl.when(c == 1)
    def _():
        tri_ref[:, :size] = jnp.zeros((size, size), jnp.float32)
        tri_ref[:, size:2 * size] = jnp.where(keep, second[:, :size], 0.0) / scaling
        tri_ref[:, 2 * size:] = product(inv1, coupled[...]) / scaling
        for q in range(2):
            y_copy(q).wait_send()

    g_drain_all(gram)
    y_drain()
    y_drain_all(coupled)
    swap_copy().wait_send()


def fused(columns):
    row_count = lax.axis_size("rows")
    width = columns.shape[1]
    scaling = math.sqrt(width * row_count)
    size = PANEL
    mates = row_count // 2
    f32 = jnp.float32
    vmem = pl.BlockSpec(memory_space=pltpu.VMEM)
    return pl.pallas_call(
        functools.partial(kernel, row_count, scaling),
        out_shape=(
            jax.ShapeDtypeStruct((size, width), f32),
            jax.ShapeDtypeStruct((size, 4 * size), f32),
            jax.ShapeDtypeStruct((size, width), f32),
        ),
        in_specs=[vmem],
        out_specs=(vmem, vmem, vmem),
        scratch_shapes=[
            pltpu.VMEM((2 * size, width), f32),
            pltpu.VMEM((2 * size, width), f32),
            pltpu.VMEM((2 * size, width), f32),
            pltpu.VMEM((3 * size, size), f32),
            pltpu.VMEM((3 * size, size), f32),
            pltpu.VMEM((3 * size // 2, size), f32),
            pltpu.VMEM((mates, 3 * size // row_count, size), f32),
            pltpu.VMEM((size, 3 * size), f32),
            pltpu.VMEM((size, 3 * size), f32),
            pltpu.VMEM((2 * size, 2 * size), f32),
            pltpu.VMEM((size, 2 * size), f32),
            pltpu.VMEM((mates, 2 * size // row_count, 2 * size), f32),
            pltpu.VMEM((2 * size // row_count, 2 * size), f32),
            pltpu.VMEM((2 * size // row_count, 2 * size), f32),
            pltpu.VMEM((2 * size, 2 * size), f32),
            pltpu.SemaphoreType.DMA((4 + 2 * (2 * mates + 2),)),
            pltpu.SemaphoreType.DMA((4,)),
            pltpu.SemaphoreType.DMA((2,)),
            pltpu.SemaphoreType.DMA((2 * mates,)),
            pltpu.SemaphoreType.DMA((2 * mates,)),
            pltpu.SemaphoreType.DMA((2,)),
            pltpu.SemaphoreType.DMA((2,)),
        ],
        compiler_params=pltpu.CompilerParams(collective_id=0, has_side_effects=True),
    )(columns)


def inverse_lower(lower):
    identity = jnp.eye(lower.shape[0], dtype=lower.dtype)
    return lax.linalg.triangular_solve(lower, identity, left_side=True, lower=True)


def summed(partial_term):
    return lax.psum(partial_term, "rows")


def general(columns):
    col_count = lax.axis_size("cols")
    col_index = lax.axis_index("cols")
    scaling = math.sqrt(columns.shape[1] * lax.axis_size("rows"))
    local_rows = lax.all_gather(columns, "cols", axis=0, tiled=True)
    panel_count = 2 * PANEL
    leading = local_rows[:panel_count]
    gram_strip = summed(product(leading, local_rows.T))
    lower_both = jnp.linalg.cholesky(gram_strip[:, :panel_count])
    inverse_both = inverse_lower(lower_both)
    orthonormal = product(inverse_both, leading)
    coupling = product(inverse_both, gram_strip[:, panel_count:])
    trailing = local_rows[panel_count:] - product(coupling.T, orthonormal)
    triangle = jnp.concatenate([lower_both.T, coupling], axis=1)
    orthonormal = orthonormal * scaling
    triangle = triangle / scaling

    def own(array):
        count = array.shape[0] // col_count
        return lax.dynamic_slice_in_dim(array, col_index * count, count, 0)

    return (own(orthonormal), own(triangle), own(trailing))


def shards(columns):
    rows = lax.axis_size("rows")
    paired = lax.axis_size("cols") == 2 and columns.shape[0] == 2 * PANEL and columns.shape[1] % (8 * PANEL) == 0
    if paired and rows % 2 == 0 and (2 * PANEL) % (8 * rows) == 0 and (3 * PANEL) % (8 * rows) == 0:
        return fused(columns)
    return general(columns)


def solution(mesh):
    placed = (P("cols", "rows"),)
    return jax.shard_map(
        shards,
        mesh=mesh,
        in_specs=placed,
        out_specs=(P("cols", "rows"), P("cols", None), P("cols", "rows")),
        check_vma=False,
    )
```

```python
import functools
import math

import jax
import jax.numpy as jnp
from jax import lax
from jax.experimental import pallas as pl
from jax.experimental.pallas import tpu as pltpu
from jax.sharding import PartitionSpec as P

PANEL = 128
STRIP = 16
VMEM_BYTES = 20 * 2**20
MESH = pl.DeviceIdType.MESH

precise = lax.Precision.HIGHEST


def product(left, right):
    return jnp.dot(left, right, precision=precise, preferred_element_type=jnp.float32)


def contract(left, right, dims):
    return lax.dot_general(
        left, right, (dims, ((), ())), precision=precise, preferred_element_type=jnp.float32
    )


def across_rows(left, right):
    return contract(left, right, ((1,), (1,)))


def pieces(value):
    first = value.astype(jnp.bfloat16)
    rest = value - first.astype(jnp.float32)
    second = rest.astype(jnp.bfloat16)
    third = (rest - second.astype(jnp.float32)).astype(jnp.bfloat16)
    return first, second, third


def strip_update(left, right):
    a, b, c = pieces(left)
    d, e, f = pieces(right)
    lhs = jnp.concatenate([a, a, b, a, c, b], axis=0)
    rhs = jnp.concatenate([d, e, d, f, d, e], axis=0)
    return lax.dot_general(
        lhs, rhs, (((0,), (0,)), ((), ())), preferred_element_type=jnp.float32
    )


def eliminate(ref, hooks):
    size = ref.shape[0]
    lanes = size
    parts = ref.shape[1] // lanes
    below = lax.broadcasted_iota(jnp.int32, (STRIP, lanes), 0)
    for s in range(size // STRIP):
        at = s * STRIP
        rows = [ref[at:at + STRIP, q * lanes:(q + 1) * lanes] for q in range(parts)]
        cols = [
            jnp.broadcast_to(rows[0][:, at + j:at + j + 1], (STRIP, lanes))
            for j in range(STRIP)
        ]
        for i in range(STRIP):
            pivot = cols[i][i:i + 1]
            inv = lax.rsqrt(pivot)
            inv = inv * (1.5 - 0.5 * pivot * inv * inv)
            col = cols[i] * inv
            coef = jnp.where(below > i, col, 0.0)
            for j in range(i + 1, STRIP):
                cols[j] = cols[j] - coef * col[j:j + 1]
            for q in range(parts):
                row = rows[q][i:i + 1] * inv
                rows[q] = jnp.where(below == i, row, rows[q] - coef * row)
        for q in range(parts):
            ref[at:at + STRIP, q * lanes:(q + 1) * lanes] = rows[q]
        after = at + STRIP
        if after < size:
            update = strip_update(rows[0], jnp.concatenate(rows, axis=1))
            ref[after:, :] = ref[after:, :] - update[after:, :]
        if s in hooks:
            hooks[s]()


def kernel(row_count, scaling, x_ref, qs, tri_ref, tail_ref, coup_ref,
           xs, ys, part, gram, pair_in, ring_in, first, second,
           xy, xy_pair, xy_ring, xy_own, xy_other, coupled, send, recv_x, recv_pair,
           recv_ring, recv_all, recv_half, recv_y):
    r = lax.axis_index("rows")
    c = lax.axis_index("cols")
    other = 1 - c
    parity = lax.rem(r, 2)
    h = r // 2
    mates = row_count // 2
    partner = (r + 1 - 2 * parity, c)
    across = (r, other)
    size = PANEL

    def mate(k):
        idx = lax.rem(h + k, mates)
        return idx, (idx * 2 + parity, c)

    barrier = pltpu.get_barrier_semaphore()
    for target in [partner, across] + [mate(k)[1] for k in range(1, mates)]:
        pl.semaphore_signal(barrier, inc=1, device_id=target, device_id_type=MESH)
    pl.semaphore_wait(barrier, mates + 1)

    def push(src, dst, send_sem, recv_sem, target):
        return pltpu.make_async_remote_copy(
            src_ref=src, dst_ref=dst, send_sem=send_sem, recv_sem=recv_sem,
            device_id=target, device_id_type=MESH)

    width = x_ref.shape[1]
    eighth = width // 8
    early = pl.ds(0, 4 * eighth)
    late = pl.ds(4 * eighth, 4 * eighth)
    spans = ((4, 3), (7, 1), (0, 3), (3, 1))

    def x_copy(q):
        span = pl.ds(spans[q][0] * eighth, spans[q][1] * eighth)
        return push(x_ref.at[:, span], xs.at[:, span], send.at[q], recv_x.at[q], across)

    def y_copy(q):
        view = (pl.ds(0, 2 * size), early) if q == 0 else (pl.ds(0, size), late)
        return push(x_ref.at[view], ys.at[view], send.at[q], recv_x.at[q], across)

    @pl.when(c == 0)
    def _():
        x_copy(0).start()

    @pl.when(c == 1)
    def _():
        y_copy(0).start()
        y_copy(1).start()
        ys[...] = x_ref[...]

    def spread(base, full, pair_buf, ring_buf, tag):
        half = full.shape[0] // 2
        chunk = half // mates
        mine = pl.ds(parity * half, half)
        his = pl.ds((1 - parity) * half, half)
        own = pl.ds(pl.multiple_of(parity * half + h * chunk, 8), chunk)

        def pair_copy():
            return push(full.at[his], pair_buf, send.at[base],
                        recv_pair.at[tag], partner)

        def ring_copy(k):
            idx, target = mate(k)
            return push(
                full.at[pl.ds(pl.multiple_of(parity * half + idx * chunk, 8), chunk)],
                ring_buf.at[k], send.at[base + k], recv_ring.at[tag * mates + k], target)

        def gather_copy(dst, k):
            return push(dst.at[own], dst.at[own], send.at[base + mates + k],
                        recv_all.at[tag * mates + k], mate(k)[1])

        def gather_wait(dst, k):
            idx = lax.rem(h + mates - k, mates)
            there = pl.ds(pl.multiple_of(parity * half + idx * chunk, 8), chunk)
            push(dst.at[there], dst.at[there], send.at[base + mates + k],
                 recv_all.at[tag * mates + k], mate(k)[1]).wait_recv()

        def half_copy(dst):
            return push(dst.at[mine], dst.at[mine], send.at[base + 2 * mates],
                        recv_half.at[tag], partner)

        def half_wait(dst):
            push(dst.at[his], dst.at[his], send.at[base + 2 * mates],
                 recv_half.at[tag], partner).wait_recv()

        def start_pair():
            pair_copy().start()

        def start_ring():
            pair_copy().wait_recv()
            full[mine] = full[mine] + pair_buf[...]
            for k in range(1, mates):
                ring_copy(k).start()

        def finish_ring():
            for k in range(1, mates):
                ring_copy(k).wait_recv()
            total = full[own]
            for k in range(1, mates):
                total = total + ring_buf[k]
            return total

        def drain_scatter():
            pair_copy().wait_send()
            for k in range(1, mates):
                ring_copy(k).wait_send()

        def start_gather(dst):
            for k in range(1, mates):
                gather_copy(dst, k).start()

        def start_half(dst):
            for k in range(1, mates):
                gather_wait(dst, k)
            half_copy(dst).start()

        def finish(dst):
            half_wait(dst)

        def drain_gather(dst):
            for k in range(1, mates):
                gather_copy(dst, k).wait_send()
            half_copy(dst).wait_send()

        return (start_pair, start_ring, finish_ring, drain_scatter, start_gather,
                start_half, finish, drain_gather, own)

    base_g = 4
    (g_pair, g_ring, g_sum, g_drain, g_gather, g_half, g_finish, g_drain_all,
     g_own) = spread(base_g, part, pair_in, ring_in, 0)
    base_y = base_g + 2 * mates + 2
    y_send = send.at[base_g + 2 * mates + 1]

    def chunk_copy():
        return push(gram.at[g_own], gram.at[g_own], y_send, recv_y.at[0], across)

    (y_pair, y_ring, y_sum, y_drain, y_gather, y_half, y_finish, y_drain_all,
     y_own) = spread(base_y, xy, xy_pair, xy_ring, 1)

    @pl.when(c == 0)
    def _():
        strip = across_rows(x_ref[:size], x_ref[...])
        part[:size] = strip[:, :size]
        part[size:2 * size] = strip[:, size:]
        part[2 * size:] = across_rows(x_ref[size:, :], x_ref[size:, :])
        g_pair()
        xs[...] = x_ref[...]
        g_ring()
        gram[g_own] = g_sum()
        chunk_copy().start()
        x_copy(1).start()
        x_copy(2).start()

    @pl.when(c == 1)
    def _():
        chunk_copy().wait_recv()

    g_gather(gram)
    g_half(gram)

    @pl.when(c == 0)
    def _():
        y_copy(0).wait_recv()
        xy[...] = across_rows(xs[:, early], ys[:, early])

    @pl.when(c == 1)
    def _():
        x_copy(0).wait_recv()
        x_copy(1).wait_recv()
        xy[...] = across_rows(xs[:, late], ys[:, late])

    y_pair()
    g_finish(gram)

    eye = (lax.broadcasted_iota(jnp.int32, (size, size), 0)
           == lax.broadcasted_iota(jnp.int32, (size, size), 1)).astype(jnp.float32)
    first[:, :size] = gram[:size]
    first[:, size:2 * size] = gram[size:2 * size]
    first[:, 2 * size:] = eye

    def swap_copy():
        return push(xy_own, xy_other, send.at[base_y + 2 * mates + 1], recv_y.at[1], across)

    def hook_sum():
        xy_own[...] = y_sum()
        swap_copy().start()

        @pl.when(c == 0)
        def _():
            x_copy(3).start()

    def hook_gather():
        swap_copy().wait_recv()
        coupled[y_own] = xy_own[...] + xy_other[...]
        y_gather(coupled)

    eliminate(first, {0: y_ring, 6: hook_sum})

    upper = first[:, size:2 * size]
    cross = contract(upper, first[:, size:], ((0,), (0,)))
    second[:, :size] = gram[2 * size:] - cross[:, :size]
    second[:, size:2 * size] = -cross[:, size:]
    second[:, 2 * size:] = eye
    eliminate(second, {0: hook_gather, 7: lambda: y_half(coupled)})

    @pl.when(c == 1)
    def _():
        x_copy(2).wait_recv()
        x_copy(3).wait_recv()

    inv00 = first[:, 2 * size:]
    inv1 = second[:, size:]
    qs[:size] = product(inv00, xs[:size])
    qs[size:] = product(inv1, xs[...])
    own_rows = pl.ds(pl.multiple_of(c * size, size), size)

    @pl.when(c == 0)
    def _():
        y_copy(1).wait_recv()

    tail_ref[...] = ys[own_rows]
    y_finish(coupled)
    mine = coupled[:, pl.ds(pl.multiple_of(c * size, size), size)]
    coup_ref[:size] = product(inv00, mine[:size])
    coup_ref[size:] = product(inv1, mine)

    keep = (lax.broadcasted_iota(jnp.int32, (size, size), 0)
            <= lax.broadcasted_iota(jnp.int32, (size, size), 1))

    @pl.when(c == 0)
    def _():
        tri_ref[:, :size] = jnp.where(keep, first[:, :size], 0.0) / scaling
        tri_ref[:, size:2 * size] = first[:, size:2 * size] / scaling
        tri_ref[:, 2 * size:] = product(inv00, coupled[:size]) / scaling
        for q in range(4):
            x_copy(q).wait_send()
        g_drain()
        chunk_copy().wait_send()

    @pl.when(c == 1)
    def _():
        tri_ref[:, :size] = jnp.zeros((size, size), jnp.float32)
        tri_ref[:, size:2 * size] = jnp.where(keep, second[:, :size], 0.0) / scaling
        tri_ref[:, 2 * size:] = product(inv1, coupled[...]) / scaling
        for q in range(2):
            y_copy(q).wait_send()

    g_drain_all(gram)
    y_drain()
    y_drain_all(coupled)
    swap_copy().wait_send()


def finish_kernel(scaling, q_ref, tri_in, tail_in, coup_ref, ortho_ref, tri_ref, trail_ref):
    size = coup_ref.shape[1]
    own_rows = pl.ds(pl.multiple_of(lax.axis_index("cols") * size, size), size)
    ortho_ref[...] = q_ref[own_rows] * scaling
    trail_ref[...] = tail_in[...] - contract(coup_ref[...], q_ref[...], ((0,), (0,)))

    @pl.when(pl.program_id(0) == 0)
    def _():
        tri_ref[...] = tri_in[...]


def fused(columns):
    row_count = lax.axis_size("rows")
    width = columns.shape[1]
    scaling = math.sqrt(width * row_count)
    size = PANEL
    mates = row_count // 2
    f32 = jnp.float32
    vmem = pl.BlockSpec(memory_space=pltpu.VMEM)
    ortho = jax.ShapeDtypeStruct((size, width), f32)
    triangle = jax.ShapeDtypeStruct((size, 4 * size), f32)
    trailing = ortho
    middle = pl.pallas_call(
        functools.partial(kernel, row_count, scaling),
        out_shape=(
            jax.ShapeDtypeStruct((2 * size, width), f32),
            triangle,
            trailing,
            jax.ShapeDtypeStruct((2 * size, size), f32),
        ),
        in_specs=[vmem],
        out_specs=(vmem, vmem, vmem, vmem),
        scratch_shapes=[
            pltpu.VMEM((2 * size, width), f32),
            pltpu.VMEM((2 * size, width), f32),
            pltpu.VMEM((3 * size, size), f32),
            pltpu.VMEM((3 * size, size), f32),
            pltpu.VMEM((3 * size // 2, size), f32),
            pltpu.VMEM((mates, 3 * size // row_count, size), f32),
            pltpu.VMEM((size, 3 * size), f32),
            pltpu.VMEM((size, 3 * size), f32),
            pltpu.VMEM((2 * size, 2 * size), f32),
            pltpu.VMEM((size, 2 * size), f32),
            pltpu.VMEM((mates, 2 * size // row_count, 2 * size), f32),
            pltpu.VMEM((2 * size // row_count, 2 * size), f32),
            pltpu.VMEM((2 * size // row_count, 2 * size), f32),
            pltpu.VMEM((2 * size, 2 * size), f32),
            pltpu.SemaphoreType.DMA((4 + 2 * (2 * mates + 2),)),
            pltpu.SemaphoreType.DMA((4,)),
            pltpu.SemaphoreType.DMA((2,)),
            pltpu.SemaphoreType.DMA((2 * mates,)),
            pltpu.SemaphoreType.DMA((2 * mates,)),
            pltpu.SemaphoreType.DMA((2,)),
            pltpu.SemaphoreType.DMA((2,)),
        ],
        compiler_params=pltpu.CompilerParams(
            collective_id=0, has_side_effects=True, vmem_limit_bytes=VMEM_BYTES),
    )(columns)
    steps = 2
    span = width // steps

    def along(rows):
        return pl.BlockSpec((rows, span), lambda i: (0, i))

    def whole(shape):
        return pl.BlockSpec(shape, lambda i: (0, 0))

    return pl.pallas_call(
        functools.partial(finish_kernel, scaling),
        grid=(steps,),
        out_shape=(ortho, triangle, trailing),
        in_specs=[along(2 * size), whole(triangle.shape), along(size), whole((2 * size, size))],
        out_specs=(along(size), whole(triangle.shape), along(size)),
        compiler_params=pltpu.CompilerParams(vmem_limit_bytes=VMEM_BYTES),
    )(*middle)


def inverse_lower(lower):
    identity = jnp.eye(lower.shape[0], dtype=lower.dtype)
    return lax.linalg.triangular_solve(lower, identity, left_side=True, lower=True)


def summed(partial_term):
    return lax.psum(partial_term, "rows")


def general(columns):
    col_count = lax.axis_size("cols")
    col_index = lax.axis_index("cols")
    scaling = math.sqrt(columns.shape[1] * lax.axis_size("rows"))
    local_rows = lax.all_gather(columns, "cols", axis=0, tiled=True)
    panel_count = 2 * PANEL
    leading = local_rows[:panel_count]
    gram_strip = summed(product(leading, local_rows.T))
    lower_both = jnp.linalg.cholesky(gram_strip[:, :panel_count])
    inverse_both = inverse_lower(lower_both)
    orthonormal = product(inverse_both, leading)
    coupling = product(inverse_both, gram_strip[:, panel_count:])
    trailing = local_rows[panel_count:] - product(coupling.T, orthonormal)
    triangle = jnp.concatenate([lower_both.T, coupling], axis=1)
    orthonormal = orthonormal * scaling
    triangle = triangle / scaling

    def own(array):
        count = array.shape[0] // col_count
        return lax.dynamic_slice_in_dim(array, col_index * count, count, 0)

    return (own(orthonormal), own(triangle), own(trailing))


def shards(columns):
    rows = lax.axis_size("rows")
    paired = lax.axis_size("cols") == 2 and columns.shape[0] == 2 * PANEL and columns.shape[1] % (8 * PANEL) == 0
    if paired and rows % 2 == 0 and (2 * PANEL) % (8 * rows) == 0 and (3 * PANEL) % (8 * rows) == 0:
        return fused(columns)
    return general(columns)


def solution(mesh):
    placed = (P("cols", "rows"),)
    return jax.shard_map(
        shards,
        mesh=mesh,
        in_specs=placed,
        out_specs=(P("cols", "rows"), P("cols", None), P("cols", "rows")),
        check_vma=False,
    )
```
